8 devices in a mesh: rep: 1 (over z), mp: 2 (over y), tb: 2 (over x), ta: 2 (over core).
Axes of the slice: x: 2, y: 2, z: 1, core: 2. Of those that a mesh axis runs over, the one named last changes fastest.
Arguments:
- x_in: bfloat16 [4096, 4096], P(('rep', 'tb', 'ta'), 'mp')
- seg_ids: int32 [4096], P(('rep', 'tb', 'ta'))
- pos_ids: int32 [4096], P(('rep', 'tb', 'ta'))
- w_q: bfloat16 [2, 4096, 4096], P(None, ('tb', 'ta'), 'mp')
- w_k: bfloat16 [2, 4096, 128], P(None, ('tb', 'ta'))
- w_v: bfloat16 [2, 4096, 128], P(None, ('tb', 'ta'))
- w_gate: bfloat16 [2, 4096, 16384], P(None, ('tb', 'ta'), 'mp')
- w_up: bfloat16 [2, 4096, 16384], P(None, ('tb', 'ta'), 'mp')
- w_out: bfloat16 [2, 4096, 4096], P(None, 'mp', ('tb', 'ta'))
- w_down: bfloat16 [2, 16384, 4096], P(None, 'mp', ('tb', 'ta'))
- norm_gain: bfloat16 [2, 4096], replicated
Outputs:
- output: float32 [4096, 4096], P(('rep', 'tb', 'ta'), 'mp')
All inputs are finite; a program needn't handle non-finite values.
Results may differ from the reference program's by a relative error of at most 0.00501459.
Values are sent between devices in bfloat16 or wider.
A program may use at most 1 GiB of HBM per device.

```python
import jax
import jax.numpy as jnp
from jax import lax

TOKENS = 4096
BLOCK_TOKENS = 1024
EMBED = 4096
HEADS = 32
HEAD_DIM = 128
FFN_DIM = 16384
LAYERS = 2
NUM_BLOCKS = TOKENS // BLOCK_TOKENS
REQ_MEAN = max(2, min(BLOCK_TOKENS // 2, 64))
ROPE_BASE = 10000.0
NORM_EPS = 1e-6


def draw_requests(key):
    starts = jax.random.randint(key, (NUM_BLOCKS, BLOCK_TOKENS), 0, REQ_MEAN) == 0
    block_start = (jnp.arange(BLOCK_TOKENS) == 0)[None, :]
    start_flags = (starts | block_start).reshape(TOKENS).astype(jnp.int32)
    tok_index = jnp.arange(TOKENS, dtype=jnp.int32)
    seg_ids = jnp.cumsum(start_flags).astype(jnp.int32) - 1
    pos_ids = tok_index - lax.cummax(start_flags * tok_index, axis=0)
    return seg_ids, pos_ids


def normal_weight(key, shape, fan_in, scale_mult):
    return (jax.random.normal(key, shape, jnp.float32) * (scale_mult * fan_in ** -0.5)).astype(jnp.bfloat16)


def setup_inputs(seed: int = 0, part: int = 0) -> dict:
    part_key = jax.random.fold_in(jax.random.key(seed), part)
    key_x, key_req = jax.random.split(part_key)
    shared = jax.random.split(jax.random.key(seed + 1), 8)
    seg_ids, pos_ids = draw_requests(key_req)
    width_q = HEADS * HEAD_DIM
    return {
        "x_in": jax.random.normal(key_x, (TOKENS, EMBED), jnp.float32).astype(jnp.bfloat16),
        "seg_ids": seg_ids,
        "pos_ids": pos_ids,
        "w_q": normal_weight(shared[0], (LAYERS, EMBED, width_q), EMBED, 1.0),
        "w_k": normal_weight(shared[1], (LAYERS, EMBED, HEAD_DIM), EMBED, 1.0),
        "w_v": normal_weight(shared[2], (LAYERS, EMBED, HEAD_DIM), EMBED, 1.0),
        "w_gate": normal_weight(shared[3], (LAYERS, EMBED, FFN_DIM), EMBED, 1.0),
        "w_up": normal_weight(shared[4], (LAYERS, EMBED, FFN_DIM), EMBED, 1.0),
        "w_out": normal_weight(shared[5], (LAYERS, width_q, EMBED), width_q, 2.0),
        "w_down": normal_weight(shared[6], (LAYERS, FFN_DIM, EMBED), FFN_DIM, 1.0),
        "norm_gain": jax.random.uniform(shared[7], (LAYERS, EMBED), jnp.float32, 0.5, 1.5).astype(jnp.bfloat16),
    }


def apply_rope(rot_in, cos_tab, sin_tab):
    half_dim = HEAD_DIM // 2
    lower_half = rot_in[..., :half_dim].astype(jnp.float32)
    upper_half = rot_in[..., half_dim:].astype(jnp.float32)
    return jnp.concatenate([lower_half * cos_tab - upper_half * sin_tab, upper_half * cos_tab + lower_half * sin_tab], axis=-1).astype(jnp.bfloat16)


def layer_block(hidden, seg_blk, pos_blk, w_q, w_k, w_v, w_gate, w_up, w_out, w_down, gain):
    mean_sq = jnp.mean(hidden * hidden, axis=-1, keepdims=True)
    normed = (hidden * lax.rsqrt(mean_sq + NORM_EPS) * gain.astype(jnp.float32)).astype(jnp.bfloat16)
    q_proj = jnp.dot(normed, w_q, preferred_element_type=jnp.float32).astype(jnp.bfloat16)
    k_proj = jnp.dot(normed, w_k, preferred_element_type=jnp.float32).astype(jnp.bfloat16)
    v_proj = jnp.dot(normed, w_v, preferred_element_type=jnp.float32).astype(jnp.bfloat16)
    gate_proj = jnp.dot(normed, w_gate, preferred_element_type=jnp.float32).astype(jnp.bfloat16)
    up_proj = jnp.dot(normed, w_up, preferred_element_type=jnp.float32).astype(jnp.bfloat16)
    half_dim = HEAD_DIM // 2
    inv_freq = ROPE_BASE ** (-(jnp.arange(half_dim, dtype=jnp.float32) * 2.0) / HEAD_DIM)
    angles = pos_blk.astype(jnp.float32)[:, None] * inv_freq[None, :]
    cos_tab = jnp.cos(angles)
    sin_tab = jnp.sin(angles)
    q_rot = apply_rope(q_proj.reshape(BLOCK_TOKENS, HEADS, HEAD_DIM), cos_tab[:, None, :], sin_tab[:, None, :])
    k_rot = apply_rope(k_proj, cos_tab, sin_tab)
    allowed = (seg_blk[:, None] == seg_blk[None, :]) & (pos_blk[None, :] <= pos_blk[:, None])
    score_scale = HEAD_DIM ** -0.5

    def one_head(q_head):
        scores = jnp.dot(q_head, k_rot.T, preferred_element_type=jnp.float32) * score_scale
        scores = jnp.where(allowed, scores, -1e30)
        row_peak = jnp.max(scores, axis=-1, keepdims=True)
        exp_scores = jnp.exp(scores - row_peak)
        prob_bf16 = (exp_scores / jnp.sum(exp_scores, axis=-1, keepdims=True)).astype(jnp.bfloat16)
        return jnp.dot(prob_bf16, v_proj, preferred_element_type=jnp.float32).astype(jnp.bfloat16)

    attn_heads = lax.map(one_head, jnp.transpose(q_rot, (1, 0, 2)))
    attn = jnp.transpose(attn_heads, (1, 0, 2)).reshape(BLOCK_TOKENS, HEADS * HEAD_DIM)
    mlp_act = (jax.nn.silu(gate_proj.astype(jnp.float32)) * up_proj.astype(jnp.float32)).astype(jnp.bfloat16)
    branch = jnp.dot(attn, w_out, preferred_element_type=jnp.float32) + jnp.dot(mlp_act, w_down, preferred_element_type=jnp.float32)
    return hidden + branch


def reference(x_in, seg_ids, pos_ids, w_q, w_k, w_v, w_gate, w_up, w_out, w_down, norm_gain):
    seg_blocks = seg_ids.reshape(NUM_BLOCKS, BLOCK_TOKENS)
    pos_blocks = pos_ids.reshape(NUM_BLOCKS, BLOCK_TOKENS)

    def layer_step(hidden, weights):
        def block_step(blk):
            return layer_block(blk[0], blk[1], blk[2], weights[0], weights[1], weights[2], weights[3], weights[4], weights[5], weights[6], weights[7])

        hidden_blocks = lax.map(block_step, (hidden.reshape(NUM_BLOCKS, BLOCK_TOKENS, EMBED), seg_blocks, pos_blocks))
        return hidden_blocks.reshape(TOKENS, EMBED), None

    final_x, unused = lax.scan(layer_step, x_in.astype(jnp.float32), (w_q, w_k, w_v, w_gate, w_up, w_out, w_down, norm_gain))
    return final_x
```

```python
import functools

import jax
import jax.numpy as jnp
from jax import lax
from jax.experimental import pallas as pl
from jax.experimental.pallas import tpu as pltpu
from jax.sharding import PartitionSpec as P


ROPE_BASE = 10000.0
NORM_EPS = 1e-6
TOKEN_AXES = ("rep", "tb", "ta")
PLANE_AXES = ("tb", "ta")
SWAP = ((0, 1), (1, 0))
CHUNKS = 4
VMEM_LIMIT = 60 * 1024 * 1024


def rope_tables(pos_ids, head_dim):
    half_dim = head_dim // 2
    inv_freq = ROPE_BASE ** (-(jnp.arange(half_dim, dtype=jnp.float32) * 2.0) / head_dim)
    angles = pos_ids.astype(jnp.float32)[:, None] * inv_freq[None, :]
    return jnp.cos(angles), jnp.sin(angles)


def apply_rope(rot_in, cos_tab, sin_tab):
    half_dim = rot_in.shape[-1] // 2
    lower_half = rot_in[..., :half_dim].astype(jnp.float32)
    upper_half = rot_in[..., half_dim:].astype(jnp.float32)
    return jnp.concatenate([lower_half * cos_tab - upper_half * sin_tab, upper_half * cos_tab + lower_half * sin_tab], axis=-1).astype(jnp.bfloat16)


def block_attention(q_rot, k_rot, v_proj, seg, pos):
    score_scale = q_rot.shape[-1] ** -0.5
    scores = jnp.einsum("thd,sd->hts", q_rot, k_rot, preferred_element_type=jnp.float32) * score_scale
    allowed = (seg[:, None] == seg[None, :]) & (pos[None, :] <= pos[:, None])
    scores = jnp.where(allowed[None], scores, -1e30)
    row_peak = jnp.max(scores, axis=-1, keepdims=True)
    exp_scores = jnp.exp(scores - row_peak)
    prob_bf16 = (exp_scores / jnp.sum(exp_scores, axis=-1, keepdims=True)).astype(jnp.bfloat16)
    return jnp.einsum("hts,sd->thd", prob_bf16, v_proj, preferred_element_type=jnp.float32).astype(jnp.bfloat16)


def hop(val, axis):
    return lax.ppermute(val, axis, SWAP)


def dot32(a, b):
    return jnp.dot(a, b, preferred_element_type=jnp.float32)


def in_kernel(gated, idx_ref, *refs):
    h_refs, refs, out_ref = refs[0:4], refs[4:-1], refs[-1]
    rows = h_refs[0].shape[1]
    for block in range(2):
        sl = slice(block * rows, (block + 1) * rows)

        def product(pieces):
            total = None
            for h_ref, piece in zip(h_refs, pieces):
                term = dot32(h_ref[block], piece[...])
                total = term if total is None else total + term
            return total.astype(jnp.bfloat16)

        if gated:
            gate = product(refs[0:4]).astype(jnp.float32)
            up = product(refs[4:8]).astype(jnp.float32)
            out_ref[sl, :] = (jax.nn.silu(gate) * up).astype(jnp.bfloat16)
        else:
            out_ref[sl, :] = product(refs[0:4])


def in_proj(idx, h, pieces, maps, n_cols, gated, tile=256):
    _, blocks, block_tok, half = h.shape
    tokens, width, depth = blocks * block_tok, 2 * half, half // 2
    once = dict(pipeline_mode=pl.Buffered(1))
    h_block = (None, blocks, block_tok, depth)
    specs = [
        pl.BlockSpec(h_block, lambda i, s: (1 - s[1], 0, 0, s[2]), **once),
        pl.BlockSpec(h_block, lambda i, s: (1 - s[1], 0, 0, 1 - s[2]), **once),
        pl.BlockSpec(h_block, lambda i, s: (s[1], 0, 0, s[2]), **once),
        pl.BlockSpec(h_block, lambda i, s: (s[1], 0, 0, 1 - s[2]), **once),
    ]
    for piece, fn in zip(pieces, maps):
        if piece.ndim == 3:
            layer, col = fn
            specs.append(pl.BlockSpec((None, depth, tile), functools.partial(lambda i, s, layer, col: (layer, 0, col(i, s)), layer=layer, col=col)))
        else:
            specs.append(pl.BlockSpec((depth, tile), functools.partial(lambda i, s, col: (0, col(i, s)), col=fn)))
    flops = 2 * tokens * width * n_cols * (2 if gated else 1)
    return pl.pallas_call(
        functools.partial(in_kernel, gated),
        grid_spec=pltpu.PrefetchScalarGridSpec(
            num_scalar_prefetch=1,
            grid=(n_cols // tile,),
            in_specs=specs,
            out_specs=pl.BlockSpec((tokens, tile), lambda i, s: (0, i)),
        ),
        out_shape=jax.ShapeDtypeStruct((tokens, n_cols), jnp.bfloat16),
        compiler_params=pltpu.CompilerParams(vmem_limit_bytes=VMEM_LIMIT),
        cost_estimate=pl.CostEstimate(flops=flops, bytes_accessed=flops // 1000, transcendentals=0),
    )(idx, h, h, h, h, *pieces)


def back_kernel(idx_ref, *refs):
    acts, weights, (send_ref, keep_ref) = refs[0:5], refs[5:13], refs[13:15]
    width = weights[0].shape[-1]
    depth = acts[0].shape[1]

    def product(wo, wd):
        total = dot32(acts[0][...], wo[...])
        for j in range(4):
            total = total + dot32(acts[1 + j][...], wd[j * depth:(j + 1) * depth, :])
        return total

    same = idx_ref[1] == 1
    first = [product(weights[0], weights[1]), product(weights[2], weights[3])]
    second = [product(weights[4], weights[5]), product(weights[6], weights[7])]

    @pl.when(same)
    def _():
        for p in range(2):
            send_ref[:, p * width:(p + 1) * width] = second[p]
            keep_ref[:, p * width:(p + 1) * width] = first[p]

    @pl.when(jnp.logical_not(same))
    def _():
        for p in range(2):
            send_ref[:, p * width:(p + 1) * width] = first[p]
            keep_ref[:, p * width:(p + 1) * width] = second[p]


def back_proj(idx, acts, w_out, w_down, own_p, recv, recv_p, layer, w, rows=256):
    tokens, depth = acts[0].shape
    width = recv[1].shape[1]
    once = dict(pipeline_mode=pl.Buffered(1))
    specs = [pl.BlockSpec((rows, depth), lambda i, s: (i, 0)) for _ in acts]
    specs.append(pl.BlockSpec((None, depth, width), lambda i, s: (layer, s[0], w), **once))
    specs.append(pl.BlockSpec((None, 4 * depth, width), lambda i, s: (layer, s[0], w), **once))
    specs.append(pl.BlockSpec((depth, width), lambda i, s: (0, w), **once))
    specs.append(pl.BlockSpec((4 * depth, width), lambda i, s: (0, w), **once))
    for _ in range(2):
        specs.append(pl.BlockSpec((depth, width), lambda i, s: (0, w), **once))
        specs.append(pl.BlockSpec((4 * depth, width), lambda i, s: (0, 0), **once))
    flops = 2 * tokens * 5 * depth * 4 * width
    out = jax.ShapeDtypeStruct((tokens, 2 * width), jnp.float32)
    return pl.pallas_call(
        back_kernel,
        grid_spec=pltpu.PrefetchScalarGridSpec(
            num_scalar_prefetch=1,
            grid=(tokens // rows,),
            in_specs=specs,
            out_specs=[pl.BlockSpec((rows, 2 * width), lambda i, s: (i, 0))] * 2,
        ),
        out_shape=[out, out],
        compiler_params=pltpu.CompilerParams(vmem_limit_bytes=VMEM_LIMIT),
        cost_estimate=pl.CostEstimate(flops=flops, bytes_accessed=flops // 1000, transcendentals=0),
    )(idx, *acts, w_out, w_down, *own_p, *recv, *recv_p)


def solution(mesh):
    def device_body(x_loc, seg_ids, pos_ids, w_q, w_k, w_v, w_gate, w_up, w_out, w_down, gain):
        tb = lax.axis_index("tb")
        ta = lax.axis_index("ta")
        mp = lax.axis_index("mp")
        num_tok, half = x_loc.shape
        quarter = half // 2
        layers = w_q.shape[0]
        head_dim = w_k.shape[-1]
        nq = w_q.shape[-1] // 2
        nf = w_gate.shape[-1] // 2
        cin = nf // CHUNKS
        cbk = w_out.shape[-1] // CHUNKS
        idx = jnp.stack([tb, (tb == mp).astype(jnp.int32), ta]).astype(jnp.int32)

        def part(w, l, r0, nr, c0, nc):
            return lax.dynamic_slice(w, (l, r0, c0), (1, nr, nc))[0]

        def gather_rows(v):
            vy = hop(v, "mp")
            vx = hop(v, "tb")
            vxy = hop(vx, "mp")
            return [[v, vx], [vy, vxy]]

        def gain_half(l, side):
            return lax.dynamic_slice_in_dim(gain[l], side * half, half).astype(jnp.float32)

        ids = jnp.stack([seg_ids, pos_ids])
        ids_f = hop(ids, "tb")
        segs, poss = (ids[0], ids_f[0]), (ids[1], ids_f[1])
        cos_tab, sin_tab = rope_tables(jnp.concatenate(poss), head_dim)
        hidden = x_loc.astype(jnp.float32)
        kv_own = jnp.concatenate([w for l in range(layers) for w in (w_k[l], w_v[l])], axis=1)
        kv_recv = hop(kv_own, "tb")
        kv_p = hop(kv_own, "ta")
        kv_e = hop(kv_recv, "ta")
        for l in range(layers):
            q_p = hop(part(w_q, l, 0, quarter, tb * nq, nq), "ta")
            g_p = hop(part(w_gate, l, 0, quarter, tb * nf, nf), "ta")
            u_p = hop(part(w_up, l, 0, quarter, tb * nf, nf), "ta")
            o_p = hop(part(w_out, l, tb * nq, nq, 0, quarter), "ta")
            d_p = hop(part(w_down, l, tb * nf, nf, 0, quarter), "ta")
            q_x = hop(part(w_q, l, 0, quarter, (1 - tb) * nq, nq), "tb")
            g_x = [hop(part(w_gate, l, 0, quarter, (1 - tb) * nf + j * cin, cin), "tb") for j in range(CHUNKS)]
            u_x = [hop(part(w_up, l, 0, quarter, (1 - tb) * nf + j * cin, cin), "tb") for j in range(CHUNKS)]
            o_x = hop(part(w_out, l, (1 - tb) * nq, nq, 0, quarter), "tb")
            d_x = [hop(part(w_down, l, (1 - tb) * nf, nf, w * cbk, cbk), "tb") for w in range(CHUNKS)]
            q_e = hop(q_x, "ta")
            g_e = [hop(g_x[j], "ta") for j in range(CHUNKS)]
            u_e = [hop(u_x[j], "ta") for j in range(CHUNKS)]
            o_e = hop(o_x, "ta")
            d_e = [hop(d_x[w], "ta") for w in range(CHUNKS)]

            if l == 0:
                full = [[v.astype(jnp.float32) for v in side] for side in gather_rows(x_loc)]
                scale = [lax.rsqrt(sum(jnp.sum(side[t] * side[t], axis=-1, keepdims=True) for side in full) / (2 * half) + NORM_EPS) for t in range(2)]
                gains = [gain_half(l, mp), gain_half(l, 1 - mp)]
                sides = [[(full[k][t] * scale[t] * gains[k]).astype(jnp.bfloat16) for t in range(2)] for k in range(2)]
            else:
                mean_sq = lax.psum(jnp.sum(hidden * hidden, axis=-1, keepdims=True), "mp") / (2 * half)
                sides = gather_rows((hidden * lax.rsqrt(mean_sq + NORM_EPS) * gain_half(l, mp)).astype(jnp.bfloat16))
            h = jnp.concatenate([v for side in sides for v in side], axis=0).reshape(2, 2, num_tok, half)

            tile = 256
            qt, ct, ft = nq // tile, cin // tile, nf // tile
            step = lambda i, s: i
            q = in_proj(idx, h, [w_q, q_p, q_x, q_e], [(l, lambda i, s: s[0] * qt + i), step, step, step], nq, False)
            kv = in_proj(idx, h, [kv_own, kv_p, kv_recv, kv_e], [lambda i, s, l=l: l] * 4, tile, False)
            q_rot = apply_rope(q.reshape(2 * num_tok, nq // head_dim, head_dim), cos_tab[:, None, :], sin_tab[:, None, :])
            k_rot = apply_rope(kv[:, :head_dim], cos_tab, sin_tab)
            v_proj = kv[:, head_dim:]
            blocks = []
            for t in range(2):
                sl = slice(t * num_tok, (t + 1) * num_tok)
                blocks.append(block_attention(q_rot[sl], k_rot[sl], v_proj[sl], segs[t], poss[t]).reshape(num_tok, nq))
            acts = [jnp.concatenate(blocks, axis=0)]
            for j in range(CHUNKS):
                own_map = (l, functools.partial(lambda i, s, j: s[0] * ft + j * ct + i, j=j))
                p_map = functools.partial(lambda i, s, j: j * ct + i, j=j)
                acts.append(in_proj(
                    idx, h, [w_gate, g_p, g_x[j], g_e[j], w_up, u_p, u_x[j], u_e[j]],
                    [own_map, p_map, step, step] * 2, cin, True))
            parts_a, parts_b = [], []
            for w in range(CHUNKS):
                send, keep = back_proj(idx, acts, w_out, w_down, (o_p, d_p), (o_x, d_x[w]), (o_e, d_e[w]), l, w)
                if w < CHUNKS - 1:
                    summed = keep + hop(send, "mp")
                    d = summed[:num_tok] + hop(summed[num_tok:], "tb")
                else:
                    passed = send[:num_tok] + hop(send[num_tok:], "tb")
                    kept = keep[:num_tok] + hop(keep[num_tok:], "tb")
                    d = kept + hop(passed, "mp")
                parts_a.append(d[:, :cbk])
                parts_b.append(d[:, cbk:])
            first = ta == 0
            pa = jnp.concatenate(parts_a, axis=1)
            pb = jnp.concatenate(parts_b, axis=1)
            hidden = hidden + jnp.concatenate([jnp.where(first, pa, pb), jnp.where(first, pb, pa)], axis=1)
        return hidden

    col_spec = P(None, PLANE_AXES, "mp")
    kv_spec = P(None, PLANE_AXES, None)
    row_spec = P(None, "mp", PLANE_AXES)
    return jax.shard_map(
        device_body,
        mesh=mesh,
        in_specs=(P(TOKEN_AXES, "mp"), P(TOKEN_AXES), P(TOKEN_AXES), col_spec, kv_spec, kv_spec, col_spec, col_spec, row_spec, row_spec, P(None, None)),
        out_specs=P(TOKEN_AXES, "mp"),
        check_vma=False,
    )
```

```python
import functools

import jax
import jax.numpy as jnp
from jax import lax
from jax.experimental import pallas as pl
from jax.experimental.pallas import tpu as pltpu
from jax.sharding import PartitionSpec as P


ROPE_BASE = 10000.0
NORM_EPS = 1e-6
TOKEN_AXES = ("rep", "tb", "ta")
PLANE_AXES = ("tb", "ta")
SWAP = ((0, 1), (1, 0))
CHUNKS = 4
VMEM_LIMIT = 60 * 1024 * 1024


def rope_tables(pos_ids, head_dim):
    half_dim = head_dim // 2
    inv_freq = ROPE_BASE ** (-(jnp.arange(half_dim, dtype=jnp.float32) * 2.0) / head_dim)
    angles = pos_ids.astype(jnp.float32)[:, None] * inv_freq[None, :]
    return jnp.cos(angles), jnp.sin(angles)


def apply_rope(rot_in, cos_tab, sin_tab):
    half_dim = rot_in.shape[-1] // 2
    lower_half = rot_in[..., :half_dim].astype(jnp.float32)
    upper_half = rot_in[..., half_dim:].astype(jnp.float32)
    return jnp.concatenate([lower_half * cos_tab - upper_half * sin_tab, upper_half * cos_tab + lower_half * sin_tab], axis=-1).astype(jnp.bfloat16)


def block_attention(q_rot, k_rot, v_proj, seg, pos):
    score_scale = q_rot.shape[-1] ** -0.5
    scores = jnp.einsum("thd,sd->hts", q_rot, k_rot, preferred_element_type=jnp.float32) * score_scale
    allowed = (seg[:, None] == seg[None, :]) & (pos[None, :] <= pos[:, None])
    scores = jnp.where(allowed[None], scores, -1e30)
    row_peak = jnp.max(scores, axis=-1, keepdims=True)
    exp_scores = jnp.exp(scores - row_peak)
    prob_bf16 = (exp_scores / jnp.sum(exp_scores, axis=-1, keepdims=True)).astype(jnp.bfloat16)
    return jnp.einsum("hts,sd->thd", prob_bf16, v_proj, preferred_element_type=jnp.float32).astype(jnp.bfloat16)


def hop(val, axis):
    return lax.ppermute(val, axis, SWAP)


def dot32(a, b):
    return jnp.dot(a, b, preferred_element_type=jnp.float32)


def in_kernel(gated, blocks, idx_ref, *refs):
    h_all, refs, out_ref = refs[0:4 * blocks], refs[4 * blocks:-1], refs[-1]
    rows = h_all[0].shape[0]
    for block in range(blocks):
        sl = slice(block * rows, (block + 1) * rows)

        def product(pieces):
            total = None
            for h_ref, piece in zip(h_all[4 * block:4 * block + 4], pieces):
                term = dot32(h_ref[...], piece[...])
                total = term if total is None else total + term
            return total.astype(jnp.bfloat16)

        if gated:
            gate = product(refs[0:4]).astype(jnp.float32)
            up = product(refs[4:8]).astype(jnp.float32)
            out_ref[sl, :] = (jax.nn.silu(gate) * up).astype(jnp.bfloat16)
        else:
            out_ref[sl, :] = product(refs[0:4])


def in_proj(idx, h, pieces, maps, n_cols, gated, tile=256):
    _, block_tok, half = h[0].shape
    tokens, width, depth = len(h) * block_tok, 2 * half, half // 2
    once = dict(pipeline_mode=pl.Buffered(1))
    h_block = (None, block_tok, depth)
    specs = [
        pl.BlockSpec(h_block, lambda i, s: (1 - s[1], 0, s[2]), **once),
        pl.BlockSpec(h_block, lambda i, s: (1 - s[1], 0, 1 - s[2]), **once),
        pl.BlockSpec(h_block, lambda i, s: (s[1], 0, s[2]), **once),
        pl.BlockSpec(h_block, lambda i, s: (s[1], 0, 1 - s[2]), **once),
    ] * len(h)
    for piece, fn in zip(pieces, maps):
        if piece.ndim == 3:
            layer, col = fn
            specs.append(pl.BlockSpec((None, depth, tile), functools.partial(lambda i, s, layer, col: (layer, 0, col(i, s)), layer=layer, col=col)))
        else:
            specs.append(pl.BlockSpec((depth, tile), functools.partial(lambda i, s, col: (0, col(i, s)), col=fn)))
    flops = 2 * tokens * width * n_cols * (2 if gated else 1)
    return pl.pallas_call(
        functools.partial(in_kernel, gated, len(h)),
        grid_spec=pltpu.PrefetchScalarGridSpec(
            num_scalar_prefetch=1,
            grid=(n_cols // tile,),
            in_specs=specs,
            out_specs=pl.BlockSpec((tokens, tile), lambda i, s: (0, i)),
        ),
        out_shape=jax.ShapeDtypeStruct((tokens, n_cols), jnp.bfloat16),
        compiler_params=pltpu.CompilerParams(vmem_limit_bytes=VMEM_LIMIT),
        cost_estimate=pl.CostEstimate(flops=flops, bytes_accessed=flops // 1000, transcendentals=0),
    )(idx, *[v for v in h for _ in range(4)], *pieces)


def back_kernel(idx_ref, *refs):
    acts, weights, (send_ref, keep_ref) = refs[0:5], refs[5:13], refs[13:15]
    width = weights[0].shape[-1]
    depth = acts[0].shape[1]

    def product(wo, wd):
        total = dot32(acts[0][...], wo[...])
        for j in range(4):
            total = total + dot32(acts[1 + j][...], wd[j * depth:(j + 1) * depth, :])
        return total

    same = idx_ref[1] == 1
    first = [product(weights[0], weights[1]), product(weights[2], weights[3])]
    second = [product(weights[4], weights[5]), product(weights[6], weights[7])]

    @pl.when(same)
    def _():
        for p in range(2):
            send_ref[:, p * width:(p + 1) * width] = second[p]
            keep_ref[:, p * width:(p + 1) * width] = first[p]

    @pl.when(jnp.logical_not(same))
    def _():
        for p in range(2):
            send_ref[:, p * width:(p + 1) * width] = first[p]
            keep_ref[:, p * width:(p + 1) * width] = second[p]


def back_proj(idx, acts, w_out, w_down, own_p, recv, recv_p, layer, w, rows=256):
    tokens, depth = acts[0].shape
    width = recv[1].shape[1]
    once = dict(pipeline_mode=pl.Buffered(1))
    specs = [pl.BlockSpec((rows, depth), lambda i, s: (i, 0)) for _ in acts]
    specs.append(pl.BlockSpec((None, depth, width), lambda i, s: (layer, s[0], w), **once))
    specs.append(pl.BlockSpec((None, 4 * depth, width), lambda i, s: (layer, s[0], w), **once))
    specs.append(pl.BlockSpec((depth, width), lambda i, s: (0, w), **once))
    specs.append(pl.BlockSpec((4 * depth, width), lambda i, s: (0, w), **once))
    for _ in range(2):
        specs.append(pl.BlockSpec((depth, width), lambda i, s: (0, w), **once))
        specs.append(pl.BlockSpec((4 * depth, width), lambda i, s: (0, 0), **once))
    flops = 2 * tokens * 5 * depth * 4 * width
    out = jax.ShapeDtypeStruct((tokens, 2 * width), jnp.float32)
    return pl.pallas_call(
        back_kernel,
        grid_spec=pltpu.PrefetchScalarGridSpec(
            num_scalar_prefetch=1,
            grid=(tokens // rows,),
            in_specs=specs,
            out_specs=[pl.BlockSpec((rows, 2 * width), lambda i, s: (i, 0))] * 2,
        ),
        out_shape=[out, out],
        compiler_params=pltpu.CompilerParams(vmem_limit_bytes=VMEM_LIMIT),
        cost_estimate=pl.CostEstimate(flops=flops, bytes_accessed=flops // 1000, transcendentals=0),
    )(idx, *acts, w_out, w_down, *own_p, *recv, *recv_p)


def split_back_kernel(idx_ref, *refs):
    out_ref, weights = refs[-1], refs[-17:-1]
    num = (len(refs) - 17) // 2
    acts = refs[:2 * num]
    width = weights[0].shape[-1]

    def product(piece):
        total = None
        for q in range(2):
            wo, wd = weights[8 * q + 2 * piece], weights[8 * q + 2 * piece + 1]
            total_q = dot32(acts[num * q][...], wo[...])
            total = total_q if total is None else total + total_q
            off = 0
            for act in acts[num * q + 1:num * (q + 1)]:
                total = total + dot32(act[...], wd[off:off + act.shape[1], :])
                off += act.shape[1]
        return total

    same = idx_ref[1] == 1
    outs = [product(p) for p in range(4)]
    for flag, order in ((same, (2, 3, 0, 1)), (jnp.logical_not(same), (0, 1, 2, 3))):
        @pl.when(flag)
        def _():
            for p in range(4):
                out_ref[:, p * width:(p + 1) * width] = outs[order[p]]


def split_back_proj(idx, acts, acts_y, w_out, w_down, mine, foreign, layer, w, rows=256):
    blocks, _, half_tok, depth = acts[0].shape
    width = mine[3].shape[1]
    tiles = half_tok // rows
    once = dict(pipeline_mode=pl.Buffered(1))
    specs = [pl.BlockSpec((None, None, rows, act.shape[-1]), lambda i, s: (i // tiles, s[3], i % tiles, 0)) for act in acts]
    specs += [pl.BlockSpec((None, rows, act.shape[-1]), lambda i, s: (i // tiles, i % tiles, 0)) for act in acts_y]
    specs.append(pl.BlockSpec((None, depth, width), lambda i, s: (layer, s[0], w), **once))
    specs.append(pl.BlockSpec((None, 4 * depth, width), lambda i, s: (layer, s[0], w), **once))
    for arr in (*mine, *foreign):
        whole = arr.shape[1] > width
        specs.append(pl.BlockSpec((arr.shape[0], width), (lambda i, s: (0, w)) if whole else (lambda i, s: (0, 0)), **once))
    flops = 2 * blocks * half_tok * 10 * depth * 4 * width
    return pl.pallas_call(
        split_back_kernel,
        grid_spec=pltpu.PrefetchScalarGridSpec(
            num_scalar_prefetch=1,
            grid=(blocks * tiles,),
            in_specs=specs,
            out_specs=pl.BlockSpec((None, rows, 4 * width), lambda i, s: (i // tiles, i % tiles, 0)),
        ),
        out_shape=jax.ShapeDtypeStruct((blocks, half_tok, 4 * width), jnp.float32),
        compiler_params=pltpu.CompilerParams(vmem_limit_bytes=VMEM_LIMIT),
        cost_estimate=pl.CostEstimate(flops=flops, bytes_accessed=flops // 1000, transcendentals=0),
    )(idx, *acts, *acts_y, w_out, w_down, *mine, *foreign)


def gu_widths(layer, hidden):
    unit = hidden // CHUNKS
    return [unit] * CHUNKS if layer == 0 else [unit] * (CHUNKS - 1) + [unit // 2] * 2


def solution(mesh):
    def device_body(x_loc, seg_ids, pos_ids, w_q, w_k, w_v, w_gate, w_up, w_out, w_down, gain):
        tb = lax.axis_index("tb")
        ta = lax.axis_index("ta")
        mp = lax.axis_index("mp")
        num_tok, half = x_loc.shape
        quarter = half // 2
        layers = w_q.shape[0]
        head_dim = w_k.shape[-1]
        nq = w_q.shape[-1] // 2
        nf = w_gate.shape[-1] // 2
        cbk = w_out.shape[-1] // CHUNKS
        idx = jnp.stack([tb, (tb == mp).astype(jnp.int32), ta, mp]).astype(jnp.int32)

        def part(w, l, r0, nr, c0, nc):
            return lax.dynamic_slice(w, (l, r0, c0), (1, nr, nc))[0]

        def gather_rows(v):
            vy = hop(v, "mp")
            vx = hop(v, "tb")
            vxy = hop(vx, "mp")
            return [[v, vx], [vy, vxy]]

        def gain_half(l, side):
            return lax.dynamic_slice_in_dim(gain[l], side * half, half).astype(jnp.float32)

        ids = jnp.stack([seg_ids, pos_ids])
        ids_f = hop(ids, "tb")
        segs, poss = (ids[0], ids_f[0]), (ids[1], ids_f[1])
        tables = [rope_tables(p, head_dim) for p in poss]
        hidden = x_loc.astype(jnp.float32)
        kv_own = jnp.concatenate([w for l in range(layers) for w in (w_k[l], w_v[l])], axis=1)
        kv_x = hop(lax.dynamic_slice_in_dim(kv_own, mp * 2 * head_dim, 2 * head_dim, axis=1), "tb")
        kv_y = hop(kv_x, "mp")
        kv_recv = jnp.where(mp == 0, jnp.concatenate([kv_x, kv_y], axis=1), jnp.concatenate([kv_y, kv_x], axis=1))
        kv_p = hop(kv_own, "ta")
        kv_e = hop(kv_recv, "ta")
        for l in range(layers):
            q_p = hop(part(w_q, l, 0, quarter, tb * nq, nq), "ta")
            g_p = hop(part(w_gate, l, 0, quarter, tb * nf, nf), "ta")
            u_p = hop(part(w_up, l, 0, quarter, tb * nf, nf), "ta")
            o_own = part(w_out, l, tb * nq, nq, 0, quarter)
            d_own = part(w_down, l, tb * nf, nf, 0, quarter)
            o_p = hop(o_own, "ta")
            d_p = hop(d_own, "ta")
            q_x = hop(part(w_q, l, 0, quarter, (1 - tb) * nq, nq), "tb")
            widths = gu_widths(l, nf)
            offs = [sum(widths[:j]) for j in range(len(widths))]
            g_x = [hop(part(w_gate, l, 0, quarter, (1 - tb) * nf + off, n), "tb") for off, n in zip(offs, widths)]
            u_x = [hop(part(w_up, l, 0, quarter, (1 - tb) * nf + off, n), "tb") for off, n in zip(offs, widths)]
            o_x = hop(part(w_out, l, (1 - tb) * nq, nq, 0, quarter), "tb")
            d_x = [hop(part(w_down, l, (1 - tb) * nf, nf, w * cbk, cbk), "tb") for w in range(CHUNKS)]
            q_e = hop(q_x, "ta")
            g_e = [hop(v, "ta") for v in g_x]
            u_e = [hop(v, "ta") for v in u_x]
            o_e = hop(o_x, "ta")
            d_e = [hop(d_x[w], "ta") for w in range(CHUNKS)]

            if l == 0:
                full = [[v.astype(jnp.float32) for v in side] for side in gather_rows(x_loc)]
                scale = [lax.rsqrt(sum(jnp.sum(side[t] * side[t], axis=-1, keepdims=True) for side in full) / (2 * half) + NORM_EPS) for t in range(2)]
                gains = [gain_half(l, mp), gain_half(l, 1 - mp)]
                sides = [[(full[k][t] * scale[t] * gains[k]).astype(jnp.bfloat16) for t in range(2)] for k in range(2)]
            else:
                mean_sq = lax.psum(jnp.sum(hidden * hidden, axis=-1, keepdims=True), "mp") / (2 * half)
                sides = gather_rows((hidden * lax.rsqrt(mean_sq + NORM_EPS) * gain_half(l, mp)).astype(jnp.bfloat16))
            h = []
            for t in range(2):
                h.append(jnp.concatenate([sides[0][t], sides[1][t]], axis=0).reshape(2, num_tok, half))

            tile = 256
            qt, ft = nq // tile, nf // tile
            step = lambda i, s: i
            blocks = []
            for t in range(2):
                q = in_proj(idx, h[t:t + 1], [w_q, q_p, q_x, q_e], [(l, lambda i, s: s[0] * qt + i), step, step, step], nq, False)
                kv = in_proj(idx, h[t:t + 1], [kv_own, kv_p, kv_recv, kv_e], [lambda i, s, l=l: l] * 4, tile, False)
                if t == 1:
                    kv, k_rot = lax.optimization_barrier((kv, k_rot))
                cos_tab, sin_tab = tables[t]
                q_rot = apply_rope(q.reshape(num_tok, nq // head_dim, head_dim), cos_tab[:, None, :], sin_tab[:, None, :])
                k_rot = apply_rope(kv[:, :head_dim], cos_tab, sin_tab)
                blocks.append(block_attention(q_rot, k_rot, kv[:, head_dim:], segs[t], poss[t]).reshape(num_tok, nq))
            acts = [jnp.concatenate(blocks, axis=0)]
            for j, (off, n) in enumerate(zip(offs, widths)):
                own_map = (l, functools.partial(lambda i, s, o: s[0] * ft + o + i, o=off // tile))
                p_map = functools.partial(lambda i, s, o: o + i, o=off // tile)
                acts.append(in_proj(
                    idx, h, [w_gate, g_p, g_x[j], g_e[j], w_up, u_p, u_x[j], u_e[j]],
                    [own_map, p_map, step, step] * 2, n, True))

            def place(res, d, w):
                for k, core in enumerate((ta, 1 - ta)):
                    col = core * quarter + w * cbk
                    part_k = lax.dynamic_slice_in_dim(res, col, cbk, axis=1) + d[:, k * cbk:(k + 1) * cbk]
                    res = lax.dynamic_update_slice_in_dim(res, part_k, col, axis=1)
                return res

            if l == layers - 1:
                half_tok = num_tok // 2
                o_y, d_y = hop(o_own, "mp"), hop(d_own, "mp")
                o_yp, d_yp = hop(o_y, "ta"), hop(d_y, "ta")
                o_xy = hop(o_x, "mp")
                o_xye = hop(o_xy, "ta")
                acts = [act.reshape(2, 2, half_tok, -1) for act in acts]
                acts_y = [hop(lax.dynamic_index_in_dim(act, 1 - mp, axis=1, keepdims=False), "mp") for act in acts]
                for w in range(CHUNKS):
                    d_xy = hop(d_x[w], "mp")
                    d_xye = hop(d_xy, "ta")
                    out = split_back_proj(idx, acts, acts_y, w_out, w_down, [o_p, d_p, o_x, d_x[w], o_e, d_e[w]], [o_y, d_y, o_yp, d_yp, o_xy, d_xy, o_xye, d_xye], l, w)
                    total = out[0] + hop(out[1], "tb")
                    kept = total[:, 2 * cbk:]
                    came = hop(total[:, :2 * cbk], "mp")
                    low = mp == 0
                    d = jnp.concatenate([jnp.where(low, kept, came), jnp.where(low, came, kept)], axis=0)
                    hidden = place(hidden, d, w)
            for w in range(CHUNKS if l < layers - 1 else 0):
                send, keep = back_proj(idx, acts, w_out, w_down, (o_p, d_p), (o_x, d_x[w]), (o_e, d_e[w]), l, w)
                summed = keep + hop(send, "mp")
                d = summed[:num_tok] + hop(summed[num_tok:], "tb")
                hidden = place(hidden, d, w)
        return hidden

    col_spec = P(None, PLANE_AXES, "mp")
    kv_spec = P(None, PLANE_AXES, None)
    row_spec = P(None, "mp", PLANE_AXES)
    return jax.shard_map(
        device_body,
        mesh=mesh,
        in_specs=(P(TOKEN_AXES, "mp"), P(TOKEN_AXES), P(TOKEN_AXES), col_spec, kv_spec, kv_spec, col_spec, col_spec, row_spec, row_spec, P(None, None)),
        out_specs=P(TOKEN_AXES, "mp"),
        check_vma=False,
    )
```
